32 devices in a mesh: facet: 4 (over y, x), col: 8 (over z, core).
Axes of the slice: x: 2, y: 2, z: 4, core: 2. Of those that a mesh axis runs over, the one named last changes fastest.
Arguments:
- facets: bfloat16 [4, 2, 768, 768], P('facet', None, 'col'), may hold values from -6 to 6
- col_offsets: int32 [8], replicated, may hold values from 0 to 767
- sub_rows: int32 [4, 8], P(None, 'col'), may hold values from 0 to 767
- facet_offsets: int32 [4, 2], replicated, may hold values from 0 to 320
- vis_pos: int32 [4, 8, 2, 256], P('facet', 'col'), may hold values from 0 to 1535
- observed: float32 [4, 8, 2, 256], P('facet', 'col'), may hold values from -6 to 6
Outputs:
- predicted: float32 [4, 8, 2, 256], P('facet', 'col')
- facet_update: float32 [4, 2, 768, 768], P('facet', None, 'col')
The draws below stay inside these ranges and needn't reach their ends.
All inputs are finite; a program needn't handle non-finite values.
Results may differ from the reference program's by a relative error of at most 0.0085.
Values may be sent and summed in bfloat16 or wider, within the bound.
A program may use at most 64 MiB of HBM per device.

```python
import math
import jax
import jax.numpy as jnp
from jax import lax

M = 64
SUB = 384
FINE = 1536
YN = 768
VIS = 256
FACETS = 4
COLS = 8
SGCOL = 4


def with_ends(result, stream_key, low, high):
    shape = result.shape
    place = [jax.random.randint(jax.random.fold_in(stream_key, axis), (), 0, shape[axis]) for axis in range(len(shape))]
    result = result.at[tuple(place)].set(low)
    longest = shape.index(max(shape))
    place[longest] = (place[longest] + 1) % shape[longest]
    return result.at[tuple(place)].set(high)


def block_scale(key, dims, shards, smallest, high):
    gain, own = 1.0, jax.random.fold_in(key, 6)
    for dim, shards_of in shards:
        heights = jnp.exp(jax.random.uniform(jax.random.fold_in(own, dim), (shards_of,), jnp.float32, smallest / len(shards), high / len(shards)))
        gain = gain * jnp.repeat(heights, dims[dim] // shards_of).reshape([-1 if axis == dim else 1 for axis in range(len(dims))])
    return gain


def normal_values(own_key, extent, scale, reach, split=(), kind=jnp.bfloat16):
    array = scale * jax.random.normal(own_key, extent, jnp.float32)
    if split:
        array = array * block_scale(own_key, extent, split, -0.22, 0.18)
    return jnp.clip(array, -reach, reach).astype(kind)


def setup_inputs(seed: int = 0) -> dict:
    streams_of = jax.random.split(jax.random.key(seed), 7)
    facets = normal_values(streams_of[0], (FACETS, 2, YN, YN), 1.0, 6.0, ((0, 4), (2, 8)))
    col_offsets = with_ends(jax.random.randint(streams_of[1], (COLS,), 0, YN), jax.random.fold_in(streams_of[1], 1), 0, YN - 1).astype(jnp.int32)
    sub_rows = with_ends(jax.random.randint(streams_of[2], (SGCOL, COLS), 0, YN), jax.random.fold_in(streams_of[2], 1), 0, YN - 1).astype(jnp.int32)
    facet_offsets = with_ends(jax.random.randint(streams_of[3], (FACETS, 2), 0, SUB - M + 1), jax.random.fold_in(streams_of[3], 1), 0, SUB - M).astype(jnp.int32)
    vis_pos = with_ends(jax.random.randint(streams_of[4], (SGCOL, COLS, 2, VIS), 0, FINE), jax.random.fold_in(streams_of[4], 1), 0, FINE - 1).astype(jnp.int32)
    observed = normal_values(streams_of[5], (SGCOL, COLS, 2, VIS), 1.0, 6.0, ((0, 4), (1, 8)), jnp.float32)
    return {"facets": facets, "col_offsets": col_offsets, "sub_rows": sub_rows, "facet_offsets": facet_offsets, "vis_pos": vis_pos, "observed": observed}


def phase_table(first_idx, second_idx, modulus, direction, factor):
    product = first_idx[:, None] * second_idx[None, :] % modulus
    angle = direction * 2.0 * math.pi / modulus * product.astype(jnp.float32)
    return (jnp.cos(angle) * factor, jnp.sin(angle) * factor)

def plain_dot(left, right):
    return jnp.dot(left, right, preferred_element_type=jnp.float32)

def lead_dot(left, right):
    return lax.dot_general(left, right, (((0,), (0,)), ((), ())), preferred_element_type=jnp.float32)

def tail_dot(left, right):
    return lax.dot_general(left, right, (((1,), (1,)), ((), ())), preferred_element_type=jnp.float32)

def batch_prod(form, left, right):
    return jnp.einsum(form, left.astype(jnp.float32), right.astype(jnp.float32), precision=lax.Precision.HIGHEST)

def place_blocks(blocks, facet_offsets, sub_count):
    zero_idx = jnp.zeros((), jnp.int32)
    canvas = jnp.zeros((2, sub_count, SUB, SUB), jnp.float32)

    def add_block(facet_idx, canvas):
        corner_at = (zero_idx, zero_idx, facet_offsets[facet_idx, 0].astype(jnp.int32), facet_offsets[facet_idx, 1].astype(jnp.int32))
        current = lax.dynamic_slice(canvas, corner_at, (2, sub_count, M, M))
        return lax.dynamic_update_slice(canvas, current + blocks[facet_idx], corner_at)
    return lax.fori_loop(0, blocks.shape[0], add_block, canvas).astype(jnp.bfloat16)

def degrid(sub_image, positions, measured):
    across = jnp.arange(SUB, dtype=jnp.int32)
    spread = 1.0 / math.sqrt(SUB)

    def one_table(points):
        return phase_table(points, across, FINE, 1.0, spread)
    u_re, u_im = jax.vmap(one_table)(positions[:, 0])
    v_re, v_im = jax.vmap(one_table)(positions[:, 1])
    u_re = u_re.astype(jnp.bfloat16)
    u_im = u_im.astype(jnp.bfloat16)
    rows_re = batch_prod('sna,sab->snb', u_re, sub_image[0]) - batch_prod('sna,sab->snb', u_im, sub_image[1])
    rows_im = batch_prod('sna,sab->snb', u_re, sub_image[1]) + batch_prod('sna,sab->snb', u_im, sub_image[0])
    pred_re = lax.optimization_barrier(jnp.sum(rows_re * v_re - rows_im * v_im, axis=2))
    pred_im = lax.optimization_barrier(jnp.sum(rows_re * v_im + rows_im * v_re, axis=2))
    predicted = jnp.stack([pred_re, pred_im], axis=1)
    diff_re = (pred_re - measured[:, 0])[:, :, None]
    diff_im = (pred_im - measured[:, 1])[:, :, None]
    weight = SUB / math.sqrt(positions.shape[2])
    wgt_re = ((diff_re * v_re + diff_im * v_im) * weight).astype(jnp.bfloat16)
    wgt_im = ((diff_im * v_re - diff_re * v_im) * weight).astype(jnp.bfloat16)
    grad_re = batch_prod('sna,snb->sab', u_re, wgt_re) + batch_prod('sna,snb->sab', u_im, wgt_im)
    grad_im = batch_prod('sna,snb->sab', u_re, wgt_im) - batch_prod('sna,snb->sab', u_im, wgt_re)
    return (predicted, jnp.stack([grad_re, grad_im]).astype(jnp.bfloat16))

def reference(facets, col_offsets, sub_rows, facet_offsets, vis_pos, observed):
    facet_count = facets.shape[0]
    sub_count = sub_rows.shape[0]
    col_count = col_offsets.shape[0]
    zero_idx = jnp.zeros((), jnp.int32)
    along_facet = jnp.arange(YN, dtype=jnp.int32)
    narrow_idx = jnp.arange(M, dtype=jnp.int32)
    inv_root = 1.0 / math.sqrt(YN)
    facet_re = facets[:, 0].reshape(facet_count * YN, YN)
    facet_im = facets[:, 1].reshape(facet_count * YN, YN)
    back_scale = math.sqrt(YN / (M * sub_count))

    def arrange(block):
        return block.reshape(sub_count, M, facet_count, M).transpose(2, 0, 1, 3)

    def regroup(block):
        return block.transpose(1, 2, 0, 3).reshape(sub_count * M, facet_count * M)

    def unfold(block):
        return block.reshape(YN, facet_count, M).transpose(1, 0, 2).reshape(facet_count * YN, M)

    def cut_blocks(gradient):

        def cut_one(offsets):
            corner_at = (zero_idx, zero_idx, offsets[0].astype(jnp.int32), offsets[1].astype(jnp.int32))
            return lax.dynamic_slice(gradient, corner_at, (2, sub_count, M, M))
        return jax.vmap(cut_one)(facet_offsets)

    def column_step(accum, column):
        w_re, w_im = phase_table(along_facet, narrow_idx + col_offsets[column], YN, -1.0, inv_root)
        w_re = w_re.astype(jnp.bfloat16)
        w_im = w_im.astype(jnp.bfloat16)
        strip_re = (plain_dot(facet_re, w_re) - plain_dot(facet_im, w_im)).astype(jnp.bfloat16)
        strip_im = (plain_dot(facet_re, w_im) + plain_dot(facet_im, w_re)).astype(jnp.bfloat16)
        strip_re = strip_re.reshape(facet_count, YN, M).transpose(1, 0, 2).reshape(YN, facet_count * M)
        strip_im = strip_im.reshape(facet_count, YN, M).transpose(1, 0, 2).reshape(YN, facet_count * M)
        targets = (narrow_idx[None, :] + sub_rows[:, column][:, None]).reshape(sub_count * M)
        e_re, e_im = phase_table(targets, along_facet, YN, -1.0, inv_root)
        e_re = e_re.astype(jnp.bfloat16)
        e_im = e_im.astype(jnp.bfloat16)
        contrib_re = (plain_dot(e_re, strip_re) - plain_dot(e_im, strip_im)).astype(jnp.bfloat16)
        contrib_im = (plain_dot(e_re, strip_im) + plain_dot(e_im, strip_re)).astype(jnp.bfloat16)
        blocks = jnp.stack([arrange(contrib_re), arrange(contrib_im)], axis=1).astype(jnp.float32)
        sub_image = place_blocks(blocks, facet_offsets, sub_count)
        predicted, gradient = degrid(sub_image, vis_pos[:, column], observed[:, column])
        backs = cut_blocks(gradient)
        back_re = regroup(backs[:, 0])
        back_im = regroup(backs[:, 1])
        delta_re = ((lead_dot(e_re, back_re) + lead_dot(e_im, back_im)) * back_scale).astype(jnp.bfloat16)
        delta_im = ((lead_dot(e_re, back_im) - lead_dot(e_im, back_re)) * back_scale).astype(jnp.bfloat16)
        delta_re = unfold(delta_re)
        delta_im = unfold(delta_im)
        add_re = tail_dot(delta_re, w_re) + tail_dot(delta_im, w_im)
        add_im = tail_dot(delta_im, w_re) - tail_dot(delta_re, w_im)
        return ((accum[0] + add_re, accum[1] + add_im), predicted)
    start_acc = (jnp.zeros((facet_count * YN, YN), jnp.float32), jnp.zeros((facet_count * YN, YN), jnp.float32))
    (acc_re, acc_im), predicted = lax.scan(column_step, start_acc, jnp.arange(col_count, dtype=jnp.int32))
    up_scale = math.sqrt(YN / (M * col_count))
    update = jnp.stack([acc_re, acc_im]).reshape(2, facet_count, YN, YN).transpose(1, 0, 2, 3) * up_scale
    return (predicted.transpose(1, 0, 2, 3), update)
```

```python
import functools
import math

import jax
import jax.numpy as jnp
from jax import lax
from jax.experimental import pallas as pl
from jax.experimental.pallas import tpu as pltpu
from jax.sharding import PartitionSpec as P

M = 64
SUB = 384
FINE = 1536
YN = 768
MESH = pl.DeviceIdType.MESH
F32 = jnp.float32
BF16 = jnp.bfloat16


def cis(product, modulus, direction):
    turns = jnp.floor(product * (1.0 / modulus) + 0.5)
    half = (product - turns * modulus) * (direction * math.pi / modulus)
    z = half * half
    s = half * (1.0 + z * (-1 / 6 + z * (1 / 120 + z * (-1 / 5040 + z * (1 / 362880 + z * (-1 / 39916800))))))
    c = 1.0 + z * (-1 / 2 + z * (1 / 24 + z * (-1 / 720 + z * (1 / 40320 + z * (-1 / 3628800 + z * (1 / 479001600))))))
    return 1.0 - 2.0 * s * s, 2.0 * s * c


def iota(shape, axis):
    return lax.broadcasted_iota(jnp.int32, shape, axis).astype(F32)


def dot(left, right, dims):
    return lax.dot_general(left, right, (dims, ((), ())), preferred_element_type=F32)


NN = ((1,), (0,))
NT = ((1,), (1,))
TN = ((0,), (0,))


def kernel(
    n_facet,
    n_col,
    facets_hbm,
    col_offsets,
    sub_rows,
    facet_offsets,
    vis_pos,
    observed,
    predicted,
    update,
    facet_buf,
    base,
    turn,
    wall,
    subt,
    subt_t,
    u_tab,
    v_tab,
    strip_out,
    strip_in,
    contrib_out,
    contrib_in,
    back_out,
    back_in,
    delta_out,
    delta_in,
    load_sem,
    col_send,
    col_recv,
    facet_send,
    facet_recv,
):
    my_f = lax.axis_index("facet")
    my_c = lax.axis_index("col")
    n_rows = facet_buf.shape[1]
    n_vis = vis_pos.shape[3]

    load = pltpu.make_async_copy(facets_hbm.at[0], facet_buf, load_sem)
    load.start()
    barrier = pltpu.get_barrier_semaphore()
    col_order = [lax.rem(my_c + n_col // 2 + i, n_col) for i in range(n_col)]
    col_order = [c for i, c in enumerate(col_order) if i != n_col // 2] + [my_c]
    facet_order = [lax.rem(my_f + 1 + i, n_facet) for i in range(n_facet)]
    for c in col_order[:-1]:
        pl.semaphore_signal(barrier, inc=1, device_id=(my_f, c), device_id_type=MESH)
    for f in facet_order[:-1]:
        pl.semaphore_signal(barrier, inc=1, device_id=(f, my_c), device_id_type=MESH)

    def col_copy(phase, out, into, slot_out, slot_in, target):
        return pltpu.make_async_remote_copy(
            src_ref=out.at[slot_out],
            dst_ref=into.at[slot_in],
            send_sem=col_send.at[phase, slot_out],
            recv_sem=col_recv.at[phase, slot_in],
            device_id=(my_f, target),
            device_id_type=MESH,
        )

    def facet_copy(phase, out, into, slot_out, slot_in, target):
        return pltpu.make_async_remote_copy(
            src_ref=out.at[slot_out],
            dst_ref=into.at[slot_in],
            send_sem=facet_send.at[phase, slot_out],
            recv_sem=facet_recv.at[phase, slot_in],
            device_id=(target, my_c),
            device_id_type=MESH,
        )

    base_re, base_im = cis(iota((M, YN), 0) * iota((M, YN), 1), YN, -1.0)
    inv_root = 1.0 / math.sqrt(YN)
    base[0] = base_re * inv_root
    base[1] = base_im * inv_root
    along = iota((1, YN), 1)
    for c in range(n_col):
        turn[0, pl.ds(c, 1)] = along * col_offsets[c].astype(F32)
    for s in range(n_facet):
        turn[0, pl.ds(n_col + s, 1)] = along * sub_rows[s, 0].astype(F32)
    turn_re, turn_im = cis(turn[0], YN, -1.0)
    turn[0] = turn_re
    turn[1] = turn_im

    def table(into, row, slot):
        re, im = turn[0, pl.ds(row, 1)], turn[1, pl.ds(row, 1)]
        into[slot, :M] = (base[0] * re - base[1] * im).astype(BF16)
        into[slot, M:] = (base[0] * im + base[1] * re).astype(BF16)

    lane = lax.broadcasted_iota(jnp.int32, (1, 2 * M), 1)
    minus_plus = jnp.where(lane < M, -1.0, 1.0)

    def swapped(value):
        return pltpu.roll(value, M, 1)

    load.wait()
    both = facet_buf[...]
    if n_rows % 16:
        both = both.astype(F32).reshape(2 * n_rows, YN).astype(BF16)
    else:
        both = both.reshape(2 * n_rows, YN)
    for i, c in enumerate(col_order):
        table(wall, c, c)
        prod = dot(both, wall[c], NT)
        part = (prod[:n_rows] + minus_plus * swapped(prod[n_rows:])).astype(BF16)
        if i == 0:
            pl.semaphore_wait(barrier, n_col - 1 + n_facet - 1)
        if i < n_col - 1:
            strip_out[c] = part
            col_copy(0, strip_out, strip_in, c, my_c, c).start()
        else:
            strip_in[c] = part

    for s in range(n_facet):
        table(subt, n_col + s, s)
    for tab, which in ((u_tab, 0), (v_tab, 1)):
        point = vis_pos[0, 0, pl.ds(which, 1)].astype(F32)
        low_re, low_im = cis(iota((M, n_vis), 0) * point, FINE, 1.0)
        low_re = low_re * (1.0 / math.sqrt(SUB))
        low_im = low_im * (1.0 / math.sqrt(SUB))
        for f in range(n_facet):
            high_re, high_im = cis(point * facet_offsets[f, which].astype(F32), FINE, 1.0)
            tab[f, :M] = (low_re * high_re - low_im * high_im).astype(tab.dtype)
            tab[f, M:] = (low_re * high_im + low_im * high_re).astype(tab.dtype)
    for s in range(n_facet):
        subt_t[:, 2 * M * s : 2 * M * (s + 1)] = subt[s].T

    for c in col_order[:-1]:
        col_copy(0, strip_out, strip_in, c, c, c).wait_recv()
    strip = strip_in[...]
    if n_rows % 16:
        strip = strip.astype(F32).reshape(YN, 2 * M).astype(BF16)
    else:
        strip = strip.reshape(YN, 2 * M)
    for i, s in enumerate(facet_order):
        prod = dot(subt[s], strip, NN)
        part = (prod[:M] + minus_plus * swapped(prod[M:])).astype(BF16)
        if i < n_facet - 1:
            contrib_out[s] = part
            facet_copy(0, contrib_out, contrib_in, s, my_f, s).start()
        else:
            contrib_in[s] = part

    pred_re = jnp.zeros((M, n_vis), F32)
    pred_im = jnp.zeros((M, n_vis), F32)
    for i in range(n_facet):
        f = facet_order[n_facet - 1 - i]
        if i > 0:
            facet_copy(0, contrib_out, contrib_in, f, f, f).wait_recv()
        with_re = dot(contrib_in[f], u_tab[f, :M], TN)
        with_im = dot(contrib_in[f], u_tab[f, M:], TN)
        rows_re = with_re[:M] - with_im[M:]
        rows_im = with_im[:M] + with_re[M:]
        v_re, v_im = v_tab[f, :M], v_tab[f, M:]
        pred_re += rows_re * v_re - rows_im * v_im
        pred_im += rows_re * v_im + rows_im * v_re
    pred_re = jnp.sum(pred_re, axis=0, keepdims=True)
    pred_im = jnp.sum(pred_im, axis=0, keepdims=True)
    predicted[0, 0, pl.ds(0, 1)] = pred_re
    predicted[0, 0, pl.ds(1, 1)] = pred_im
    weight = SUB / math.sqrt(n_vis)
    diff_re = pred_re - observed[0, 0, pl.ds(0, 1)]
    diff_im = pred_im - observed[0, 0, pl.ds(1, 1)]
    for i, f in enumerate(facet_order):
        v_re, v_im = v_tab[f, :M], v_tab[f, M:]
        wgt_re = ((diff_re * v_re + diff_im * v_im) * weight).astype(BF16)
        wgt_im = ((diff_im * v_re - diff_re * v_im) * weight).astype(BF16)
        prod = dot(u_tab[f], jnp.concatenate([wgt_re, wgt_im], axis=0), NT)
        part = (prod[:M] - minus_plus * swapped(prod[M:])).astype(BF16)
        if i < n_facet - 1:
            back_out[f] = part
            facet_copy(1, back_out, back_in, f, my_f, f).start()
        else:
            back_in[f] = part

    for s in facet_order[:-1]:
        facet_copy(1, back_out, back_in, s, s, s).wait_recv()
    stacked = []
    for s in range(n_facet):
        block = back_in[s]
        stacked += [block, (-minus_plus * swapped(block.astype(F32))).astype(BF16)]
    back_scale = math.sqrt(YN / (M * n_facet))
    delta = dot(subt_t[...], jnp.concatenate(stacked, axis=0), NN) * back_scale
    delta_out[...] = delta.reshape(n_col, n_rows, 2 * M).astype(BF16)
    for c in col_order[:-1]:
        col_copy(1, delta_out, delta_in, c, my_c, c).start()
    delta_in[my_c] = delta_out[my_c]

    for c in col_order[:-1]:
        col_copy(1, delta_out, delta_in, c, c, c).wait_recv()
    up_scale = math.sqrt(YN / (M * n_col))
    straight, crossed = [], []
    for c in range(n_col):
        block = delta_in[c]
        straight.append(block)
        crossed.append((-minus_plus * swapped(block.astype(F32))).astype(BF16))
    straight = jnp.concatenate(straight, axis=1)
    crossed = jnp.concatenate(crossed, axis=1)
    full = wall[...].reshape(n_col * 2 * M, YN)
    update[0, 0] = dot(straight, full, NN) * up_scale
    update[0, 1] = dot(crossed, full, NN) * up_scale

    for c in col_order[:-1]:
        col_copy(0, strip_out, strip_in, c, c, c).wait_send()
        col_copy(1, delta_out, delta_in, c, c, c).wait_send()
    for f in facet_order[:-1]:
        facet_copy(0, contrib_out, contrib_in, f, f, f).wait_send()
        facet_copy(1, back_out, back_in, f, f, f).wait_send()


def body(n_facet, n_col, facets, col_offsets, sub_rows, facet_offsets, vis_pos, observed):
    assert sub_rows.shape[0] == n_facet
    n_rows = facets.shape[2]
    n_vis = vis_pos.shape[3]
    vmem = pl.BlockSpec(memory_space=pltpu.VMEM)
    smem = pl.BlockSpec(memory_space=pltpu.SMEM)
    facet_blocks = pltpu.VMEM((n_facet, M, 2 * M), BF16)
    col_blocks = pltpu.VMEM((n_col, n_rows, 2 * M), BF16)
    table_rows = n_col + n_facet
    return tuple(
        pl.pallas_call(
            functools.partial(kernel, n_facet, n_col),
            out_shape=(
                jax.ShapeDtypeStruct(observed.shape, F32),
                jax.ShapeDtypeStruct(facets.shape, F32),
            ),
            in_specs=[pl.BlockSpec(memory_space=pl.ANY), smem, smem, smem, vmem, vmem],
            out_specs=(vmem, vmem),
            scratch_shapes=[
                pltpu.VMEM((2, n_rows, YN), BF16),
                pltpu.VMEM((2, M, YN), F32),
                pltpu.VMEM((2, table_rows, YN), F32),
                pltpu.VMEM((n_col, 2 * M, YN), BF16),
                pltpu.VMEM((n_facet, 2 * M, YN), BF16),
                pltpu.VMEM((YN, n_facet * 2 * M), BF16),
                pltpu.VMEM((n_facet, 2 * M, n_vis), BF16),
                pltpu.VMEM((n_facet, 2 * M, n_vis), F32),
                col_blocks,
                col_blocks,
                facet_blocks,
                facet_blocks,
                facet_blocks,
                facet_blocks,
                col_blocks,
                col_blocks,
                pltpu.SemaphoreType.DMA,
                pltpu.SemaphoreType.DMA((2, n_col)),
                pltpu.SemaphoreType.DMA((2, n_col)),
                pltpu.SemaphoreType.DMA((2, n_facet)),
                pltpu.SemaphoreType.DMA((2, n_facet)),
            ],
            compiler_params=pltpu.CompilerParams(collective_id=0, has_side_effects=True),
            name="predict_update",
        )(facets, col_offsets, sub_rows, facet_offsets, vis_pos, observed)
    )


def solution(mesh):
    in_specs = (
        P("facet", None, "col", None),
        P(),
        P(None, "col"),
        P(),
        P("facet", "col", None, None),
        P("facet", "col", None, None),
    )
    out_specs = (P("facet", "col", None, None), P("facet", None, "col", None))
    step = functools.partial(body, mesh.shape["facet"], mesh.shape["col"])
    return jax.shard_map(step, mesh=mesh, in_specs=in_specs, out_specs=out_specs, check_vma=False)
```

```python
import functools
import math

import jax
import jax.numpy as jnp
from jax import lax
from jax.experimental import pallas as pl
from jax.experimental.pallas import tpu as pltpu
from jax.sharding import PartitionSpec as P

M = 64
SUB = 384
FINE = 1536
YN = 768
MARGIN = 8192
MESH = pl.DeviceIdType.MESH
F32 = jnp.float32
BF16 = jnp.bfloat16


def cis(product, modulus, direction):
    turns = jnp.floor(product * (1.0 / modulus) + 0.5)
    half = (product - turns * modulus) * (direction * math.pi / modulus)
    z = half * half
    s = half * (1.0 + z * (-1 / 6 + z * (1 / 120 + z * (-1 / 5040 + z * (1 / 362880 + z * (-1 / 39916800))))))
    c = 1.0 + z * (-1 / 2 + z * (1 / 24 + z * (-1 / 720 + z * (1 / 40320 + z * (-1 / 3628800 + z * (1 / 479001600))))))
    return 1.0 - 2.0 * s * s, 2.0 * s * c


def iota(shape, axis):
    return lax.broadcasted_iota(jnp.int32, shape, axis).astype(F32)


def dot(left, right, dims):
    return lax.dot_general(left, right, (dims, ((), ())), preferred_element_type=F32)


NN = ((1,), (0,))
NT = ((1,), (1,))
TN = ((0,), (0,))


def kernel(
    n_facet,
    n_col,
    facets_hbm,
    col_offsets_hbm,
    sub_rows_hbm,
    facet_offsets_hbm,
    vis_pos_hbm,
    observed_hbm,
    predicted,
    update,
    facet_buf,
    col_offsets,
    sub_rows,
    facet_offsets,
    vis_pos,
    observed,
    base,
    turn,
    wall,
    subt,
    subt_t,
    u_tab,
    v_tab,
    strip_out,
    strip_in,
    contrib_out,
    contrib_in,
    back_out,
    back_in,
    delta_out,
    delta_in,
    load_sem,
    col_send,
    col_recv,
    facet_send,
    facet_recv,
):
    my_f = lax.axis_index("facet")
    my_c = lax.axis_index("col")
    n_rows = facet_buf.shape[1]
    n_vis = vis_pos.shape[3]

    loads = [
        pltpu.make_async_copy(source, held, load_sem.at[i])
        for i, (source, held) in enumerate(
            (
                (col_offsets_hbm, col_offsets),
                (sub_rows_hbm, sub_rows),
                (facets_hbm.at[0], facet_buf),
                (facet_offsets_hbm, facet_offsets),
                (vis_pos_hbm, vis_pos),
                (observed_hbm, observed),
            )
        )
    ]
    for load in loads:
        load.start()
    barrier = pltpu.get_barrier_semaphore()
    n_pair = n_col // 2
    my_pair, my_core = my_c // 2, lax.rem(my_c, 2)
    steps = sorted(range(1, n_pair), key=lambda step: -min(step, n_pair - step)) + [0]
    pair_order = [lax.rem(my_pair + step, n_pair) for step in steps]
    col_order = []
    for pair in pair_order:
        col_order += [2 * pair + 1 - my_core, 2 * pair + my_core]
    facet_order = [lax.rem(my_f + 1 + i, n_facet) for i in range(n_facet)]
    for c in col_order[:-1]:
        pl.semaphore_signal(barrier, inc=1, device_id=(my_f, c), device_id_type=MESH)
    for f in facet_order[:-1]:
        pl.semaphore_signal(barrier, inc=1, device_id=(f, my_c), device_id_type=MESH)

    def col_copy(phase, out, into, slot_out, slot_in, target):
        return pltpu.make_async_remote_copy(
            src_ref=out.at[slot_out],
            dst_ref=into.at[slot_in],
            send_sem=col_send.at[phase, slot_out],
            recv_sem=col_recv.at[phase, slot_in],
            device_id=(my_f, target),
            device_id_type=MESH,
        )

    def facet_copy(phase, out, into, slot_out, slot_in, target):
        return pltpu.make_async_remote_copy(
            src_ref=out.at[slot_out],
            dst_ref=into.at[slot_in],
            send_sem=facet_send.at[phase, slot_out],
            recv_sem=facet_recv.at[phase, slot_in],
            device_id=(target, my_c),
            device_id_type=MESH,
        )

    base_re, base_im = cis(iota((M, YN), 0) * iota((M, YN), 1), YN, -1.0)
    inv_root = 1.0 / math.sqrt(YN)
    base[0] = base_re * inv_root
    base[1] = base_im * inv_root
    along = iota((1, YN), 1)
    loads[0].wait()
    loads[1].wait()
    for c in range(n_col):
        turn[0, pl.ds(c, 1)] = along * col_offsets[c].astype(F32)
    for s in range(n_facet):
        turn[0, pl.ds(n_col + s, 1)] = along * sub_rows[0, s].astype(F32)
    turn_re, turn_im = cis(turn[0], YN, -1.0)
    turn[0] = turn_re
    turn[1] = turn_im

    def table(into, row, slot):
        re, im = turn[0, pl.ds(row, 1)], turn[1, pl.ds(row, 1)]
        into[slot, :M] = (base[0] * re - base[1] * im).astype(BF16)
        into[slot, M:] = (base[0] * im + base[1] * re).astype(BF16)

    lane = lax.broadcasted_iota(jnp.int32, (1, 2 * M), 1)
    minus_plus = jnp.where(lane < M, -1.0, 1.0)

    def swapped(value):
        return pltpu.roll(value, M, 1)

    loads[2].wait()
    both = facet_buf[...]
    if n_rows % 16:
        both = both.astype(F32).reshape(2 * n_rows, YN).astype(BF16)
    else:
        both = both.reshape(2 * n_rows, YN)
    early = n_col // 2
    for i, c in enumerate(col_order):
        table(wall, c, c)
        prod = dot(both, wall[c], NT)
        part = (prod[:n_rows] + minus_plus * swapped(prod[n_rows:])).astype(BF16)
        if i < n_col - 1:
            strip_out[c] = part
        else:
            strip_in[c] = part
        if i == early - 1:
            pl.semaphore_wait(barrier, n_col - 1 + n_facet - 1)
            for ready in col_order[:early]:
                col_copy(0, strip_out, strip_in, ready, my_c, ready).start()
        elif early <= i < n_col - 1:
            col_copy(0, strip_out, strip_in, c, my_c, c).start()

    for s in range(n_facet):
        table(subt, n_col + s, s)
    for load in loads[3:]:
        load.wait()
    for tab, which in ((u_tab, 0), (v_tab, 1)):
        point = vis_pos[0, 0, pl.ds(which, 1)].astype(F32)
        low_re, low_im = cis(iota((M, n_vis), 0) * point, FINE, 1.0)
        low_re = low_re * (1.0 / math.sqrt(SUB))
        low_im = low_im * (1.0 / math.sqrt(SUB))
        for f in range(n_facet):
            high_re, high_im = cis(point * facet_offsets[which, f].astype(F32), FINE, 1.0)
            tab[f, :M] = (low_re * high_re - low_im * high_im).astype(tab.dtype)
            tab[f, M:] = (low_re * high_im + low_im * high_re).astype(tab.dtype)
    for s in range(n_facet):
        subt_t[:, 2 * M * s : 2 * M * (s + 1)] = subt[s].T

    for c in col_order[:-1]:
        col_copy(0, strip_out, strip_in, c, c, c).wait_recv()
    strip = strip_in[...]
    if n_rows % 16:
        strip = strip.astype(F32).reshape(YN, 2 * M).astype(BF16)
    else:
        strip = strip.reshape(YN, 2 * M)
    prod = dot(subt[...].reshape(n_facet * 2 * M, YN), strip, NN)
    for s in range(n_facet):
        top = prod[2 * M * s : 2 * M * s + M]
        low = prod[2 * M * s + M : 2 * M * (s + 1)]
        contrib_out[s] = (top + minus_plus * swapped(low)).astype(BF16)
    for s in facet_order[:-1]:
        facet_copy(0, contrib_out, contrib_in, s, my_f, s).start()
    contrib_in[my_f] = contrib_out[my_f]

    pred_re = jnp.zeros((M, n_vis), F32)
    pred_im = jnp.zeros((M, n_vis), F32)
    for i in range(n_facet):
        f = facet_order[n_facet - 1 - i]
        if i > 0:
            facet_copy(0, contrib_out, contrib_in, f, f, f).wait_recv()
        with_re = dot(contrib_in[f], u_tab[f, :M], TN)
        with_im = dot(contrib_in[f], u_tab[f, M:], TN)
        rows_re = with_re[:M] - with_im[M:]
        rows_im = with_im[:M] + with_re[M:]
        v_re, v_im = v_tab[f, :M], v_tab[f, M:]
        pred_re += rows_re * v_re - rows_im * v_im
        pred_im += rows_re * v_im + rows_im * v_re
    pred_re = jnp.sum(pred_re, axis=0, keepdims=True)
    pred_im = jnp.sum(pred_im, axis=0, keepdims=True)
    predicted[0, 0, pl.ds(0, 1)] = pred_re
    predicted[0, 0, pl.ds(1, 1)] = pred_im
    weight = SUB / math.sqrt(n_vis)
    diff_re = pred_re - observed[0, 0, pl.ds(0, 1)]
    diff_im = pred_im - observed[0, 0, pl.ds(1, 1)]
    for i, f in enumerate(facet_order):
        v_re, v_im = v_tab[f, :M], v_tab[f, M:]
        wgt_re = ((diff_re * v_re + diff_im * v_im) * weight).astype(BF16)
        wgt_im = ((diff_im * v_re - diff_re * v_im) * weight).astype(BF16)
        prod = dot(u_tab[f], jnp.concatenate([wgt_re, wgt_im], axis=0), NT)
        part = (prod[:M] - minus_plus * swapped(prod[M:])).astype(BF16)
        if i < n_facet - 1:
            back_out[f] = part
            facet_copy(1, back_out, back_in, f, my_f, f).start()
        else:
            back_in[f] = part

    for s in facet_order[:-1]:
        facet_copy(1, back_out, back_in, s, s, s).wait_recv()
    stacked = []
    for s in range(n_facet):
        block = back_in[s]
        stacked += [block, (-minus_plus * swapped(block.astype(F32))).astype(BF16)]
    back_scale = math.sqrt(YN / (M * n_facet))
    stacked = jnp.concatenate(stacked, axis=0)
    for i, pair in enumerate(pair_order):
        start = pl.multiple_of(pair * (2 * n_rows), 2 * n_rows)
        delta = dot(subt_t[pl.ds(start, 2 * n_rows)], stacked, NN) * back_scale
        delta_out[pl.ds(2 * pair, 2)] = delta.reshape(2, n_rows, 2 * M).astype(BF16)
        for c in col_order[2 * i : 2 * i + 2]:
            if c is not col_order[-1]:
                col_copy(1, delta_out, delta_in, c, my_c, c).start()
    delta_in[my_c] = delta_out[my_c]

    up_scale = math.sqrt(YN / (M * n_col))
    for i in reversed(range(n_pair)):
        for c in col_order[2 * i : 2 * i + 2]:
            if c is not col_order[-1]:
                col_copy(1, delta_out, delta_in, c, c, c).wait_recv()
        pair = pair_order[i]
        blocks = [delta_in[2 * pair + core] for core in range(2)]
        turned = [(-minus_plus * swapped(block.astype(F32))).astype(BF16) for block in blocks]
        walls = wall[pl.ds(2 * pair, 2)].reshape(4 * M, YN)
        for part, sides in enumerate((blocks, turned)):
            term = dot(jnp.concatenate(sides, axis=1), walls, NN)
            if i < n_pair - 1:
                term += update[0, part]
            update[0, part] = term * up_scale if i == 0 else term

    for c in col_order[:-1]:
        col_copy(0, strip_out, strip_in, c, c, c).wait_send()
        col_copy(1, delta_out, delta_in, c, c, c).wait_send()
    for f in facet_order[:-1]:
        facet_copy(0, contrib_out, contrib_in, f, f, f).wait_send()
        facet_copy(1, back_out, back_in, f, f, f).wait_send()


def deliver_kernel(predicted, update, predicted_hbm, update_hbm, sems):
    copies = [
        pltpu.make_async_copy(update, update_hbm, sems.at[0]),
        pltpu.make_async_copy(predicted, predicted_hbm, sems.at[1]),
    ]
    for copy in copies:
        copy.start()
    for copy in copies:
        copy.wait()


def deliver(predicted, update):
    vmem = pl.BlockSpec(memory_space=pltpu.VMEM)
    hbm = pl.BlockSpec(memory_space=pltpu.HBM)
    return pl.pallas_call(
        deliver_kernel,
        out_shape=(
            jax.ShapeDtypeStruct(predicted.shape, F32),
            jax.ShapeDtypeStruct(update.shape, F32),
        ),
        in_specs=[vmem, vmem],
        out_specs=(hbm, hbm),
        scratch_shapes=[pltpu.SemaphoreType.DMA((2,))],
        compiler_params=pltpu.CompilerParams(vmem_limit_bytes=2**20),
        name="deliver",
    )(predicted, update)


def body(n_facet, n_col, facets, col_offsets, sub_rows, facet_offsets, vis_pos, observed):
    assert sub_rows.shape[0] == n_facet
    n_rows = facets.shape[2]
    n_vis = vis_pos.shape[3]
    vmem = pl.BlockSpec(memory_space=pltpu.VMEM)
    facet_blocks = pltpu.VMEM((n_facet, M, 2 * M), BF16)
    col_blocks = pltpu.VMEM((n_col, n_rows, 2 * M), BF16)
    table_rows = n_col + n_facet
    vmem_left = (67043328 - 4 * (facets.size + observed.size)) // 1024 * 1024 - MARGIN
    results = pl.pallas_call(
            functools.partial(kernel, n_facet, n_col),
            out_shape=(pltpu.VMEM(observed.shape, F32), pltpu.VMEM(facets.shape, F32)),
            in_specs=[pl.BlockSpec(memory_space=pltpu.HBM)] * 6,
            out_specs=(vmem, vmem),
            scratch_shapes=[
                pltpu.VMEM((2, n_rows, YN), BF16),
                pltpu.SMEM(col_offsets.shape, jnp.int32),
                pltpu.SMEM(sub_rows.shape[::-1], jnp.int32),
                pltpu.SMEM(facet_offsets.shape[::-1], jnp.int32),
                pltpu.VMEM(vis_pos.shape, jnp.int32),
                pltpu.VMEM(observed.shape, F32),
                pltpu.VMEM((2, M, YN), F32),
                pltpu.VMEM((2, table_rows, YN), F32),
                pltpu.VMEM((n_col, 2 * M, YN), BF16),
                pltpu.VMEM((n_facet, 2 * M, YN), BF16),
                pltpu.VMEM((YN, n_facet * 2 * M), BF16),
                pltpu.VMEM((n_facet, 2 * M, n_vis), BF16),
                pltpu.VMEM((n_facet, 2 * M, n_vis), F32),
                col_blocks,
                col_blocks,
                facet_blocks,
                facet_blocks,
                facet_blocks,
                facet_blocks,
                col_blocks,
                col_blocks,
                pltpu.SemaphoreType.DMA((6,)),
                pltpu.SemaphoreType.DMA((2, n_col)),
                pltpu.SemaphoreType.DMA((2, n_col)),
                pltpu.SemaphoreType.DMA((2, n_facet)),
                pltpu.SemaphoreType.DMA((2, n_facet)),
            ],
            compiler_params=pltpu.CompilerParams(
                collective_id=0, has_side_effects=True, vmem_limit_bytes=vmem_left
            ),
            name="predict_update",
        )(facets, col_offsets, sub_rows.T, facet_offsets.T, vis_pos, observed)
    return deliver(*results)


def solution(mesh):
    in_specs = (
        P("facet", None, "col", None),
        P(),
        P(None, "col"),
        P(),
        P("facet", "col", None, None),
        P("facet", "col", None, None),
    )
    out_specs = (P("facet", "col", None, None), P("facet", None, "col", None))
    step = functools.partial(body, mesh.shape["facet"], mesh.shape["col"])
    return jax.shard_map(step, mesh=mesh, in_specs=in_specs, out_specs=out_specs, check_vma=False)
```

```python
import functools
import math

import jax
import jax.numpy as jnp
from jax import lax
from jax.experimental import pallas as pl
from jax.experimental.pallas import tpu as pltpu
from jax.sharding import PartitionSpec as P

M = 64
SUB = 384
FINE = 1536
YN = 768
MARGIN = 8192
MESH = pl.DeviceIdType.MESH
F32 = jnp.float32
BF16 = jnp.bfloat16


def cis(product, modulus, direction):
    turns = jnp.floor(product * (1.0 / modulus) + 0.5)
    half = (product - turns * modulus) * (direction * math.pi / modulus)
    z = half * half
    s = half * (1.0 + z * (-1 / 6 + z * (1 / 120 + z * (-1 / 5040 + z * (1 / 362880 + z * (-1 / 39916800))))))
    c = 1.0 + z * (-1 / 2 + z * (1 / 24 + z * (-1 / 720 + z * (1 / 40320 + z * (-1 / 3628800 + z * (1 / 479001600))))))
    return 1.0 - 2.0 * s * s, 2.0 * s * c


def iota(shape, axis):
    return lax.broadcasted_iota(jnp.int32, shape, axis).astype(F32)


def dot(left, right, dims):
    return lax.dot_general(left, right, (dims, ((), ())), preferred_element_type=F32)


NN = ((1,), (0,))
NT = ((1,), (1,))
TN = ((0,), (0,))


def kernel(
    n_facet,
    n_col,
    facets_hbm,
    col_offsets_hbm,
    sub_rows_hbm,
    facet_offsets_hbm,
    vis_pos_hbm,
    observed_hbm,
    predicted,
    update,
    facet_buf,
    col_offsets,
    sub_rows,
    facet_offsets,
    vis_pos,
    observed,
    base,
    turn,
    wall,
    subt,
    subt_t,
    u_tab,
    v_tab,
    strip_out,
    strip_in,
    contrib_out,
    contrib_in,
    back_out,
    back_in,
    delta_out,
    delta_in,
    load_sem,
    col_send,
    col_recv,
    facet_send,
    facet_recv,
):
    my_f = lax.axis_index("facet")
    my_c = lax.axis_index("col")
    n_rows = facet_buf.shape[1]
    n_vis = vis_pos.shape[3]

    loads = [
        pltpu.make_async_copy(source, held, load_sem.at[i])
        for i, (source, held) in enumerate(
            (
                (col_offsets_hbm, col_offsets),
                (sub_rows_hbm, sub_rows),
                (facets_hbm.at[0], facet_buf),
                (facet_offsets_hbm, facet_offsets),
                (vis_pos_hbm, vis_pos),
                (observed_hbm, observed),
            )
        )
    ]
    for load in loads:
        load.start()
    barrier = pltpu.get_barrier_semaphore()
    n_pair = n_col // 2
    my_pair, my_core = my_c // 2, lax.rem(my_c, 2)
    side = my_pair // (n_pair // 2)
    mirrored = my_pair + side * (n_pair - 1 - 2 * my_pair)
    pair_order = []
    for place in range(n_pair - 1, 0, -1):
        target = place - (mirrored + n_pair - place) // n_pair
        pair_order.append(target + side * (n_pair - 1 - 2 * target))
    pair_order.append(my_pair)
    col_order = []
    for pair in pair_order:
        col_order += [2 * pair + 1 - my_core, 2 * pair + my_core]
    facet_order = [lax.rem(my_f + 1 + i, n_facet) for i in range(n_facet)]
    for c in col_order[:-1]:
        pl.semaphore_signal(barrier, inc=1, device_id=(my_f, c), device_id_type=MESH)
    for f in facet_order[:-1]:
        pl.semaphore_signal(barrier, inc=1, device_id=(f, my_c), device_id_type=MESH)

    def col_copy(phase, out, into, slot_out, slot_in, target):
        return pltpu.make_async_remote_copy(
            src_ref=out.at[slot_out],
            dst_ref=into.at[slot_in],
            send_sem=col_send.at[phase, slot_out],
            recv_sem=col_recv.at[phase, slot_in],
            device_id=(my_f, target),
            device_id_type=MESH,
        )

    def facet_copy(phase, out, into, slot_out, slot_in, target):
        return pltpu.make_async_remote_copy(
            src_ref=out.at[slot_out],
            dst_ref=into.at[slot_in],
            send_sem=facet_send.at[phase, slot_out],
            recv_sem=facet_recv.at[phase, slot_in],
            device_id=(target, my_c),
            device_id_type=MESH,
        )

    base_re, base_im = cis(iota((M, YN), 0) * iota((M, YN), 1), YN, -1.0)
    inv_root = 1.0 / math.sqrt(YN)
    base[0] = base_re * inv_root
    base[1] = base_im * inv_root
    along = iota((1, YN), 1)
    loads[0].wait()
    loads[1].wait()
    for c in range(n_col):
        turn[0, pl.ds(c, 1)] = along * col_offsets[c].astype(F32)
    for s in range(n_facet):
        turn[0, pl.ds(n_col + s, 1)] = along * sub_rows[0, s].astype(F32)
    turn_re, turn_im = cis(turn[0], YN, -1.0)
    turn[0] = turn_re
    turn[1] = turn_im

    def table(into, row, slot):
        re, im = turn[0, pl.ds(row, 1)], turn[1, pl.ds(row, 1)]
        into[slot, :M] = (base[0] * re - base[1] * im).astype(BF16)
        into[slot, M:] = (base[0] * im + base[1] * re).astype(BF16)

    lane = lax.broadcasted_iota(jnp.int32, (1, 2 * M), 1)
    minus_plus = jnp.where(lane < M, -1.0, 1.0)

    def swapped(value):
        return pltpu.roll(value, M, 1)

    loads[2].wait()
    both = facet_buf[...]
    if n_rows % 16:
        both = both.astype(F32).reshape(2 * n_rows, YN).astype(BF16)
    else:
        both = both.reshape(2 * n_rows, YN)
    early = n_col - 1
    for i, c in enumerate(col_order):
        table(wall, c, c)
        prod = dot(both, wall[c], NT)
        part = (prod[:n_rows] + minus_plus * swapped(prod[n_rows:])).astype(BF16)
        if i < n_col - 1:
            strip_out[c] = part
        else:
            strip_in[c] = part
        if i == early - 1:
            pl.semaphore_wait(barrier, n_col - 1 + n_facet - 1)
            for ready in col_order[:early]:
                col_copy(0, strip_out, strip_in, ready, my_c, ready).start()
        elif early <= i < n_col - 1:
            col_copy(0, strip_out, strip_in, c, my_c, c).start()

    for s in range(n_facet):
        table(subt, n_col + s, s)
    for load in loads[3:]:
        load.wait()
    for tab, which in ((u_tab, 0), (v_tab, 1)):
        point = vis_pos[0, 0, pl.ds(which, 1)].astype(F32)
        low_re, low_im = cis(iota((M, n_vis), 0) * point, FINE, 1.0)
        low_re = low_re * (1.0 / math.sqrt(SUB))
        low_im = low_im * (1.0 / math.sqrt(SUB))
        for f in range(n_facet):
            high_re, high_im = cis(point * facet_offsets[which, f].astype(F32), FINE, 1.0)
            tab[f, :M] = (low_re * high_re - low_im * high_im).astype(tab.dtype)
            tab[f, M:] = (low_re * high_im + low_im * high_re).astype(tab.dtype)
    for s in range(n_facet):
        subt_t[:, 2 * M * s : 2 * M * (s + 1)] = subt[s].T

    for c in col_order[:-1]:
        col_copy(0, strip_out, strip_in, c, c, c).wait_recv()
    strip = strip_in[...]
    if n_rows % 16:
        strip = strip.astype(F32).reshape(YN, 2 * M).astype(BF16)
    else:
        strip = strip.reshape(YN, 2 * M)
    prod = dot(subt[...].reshape(n_facet * 2 * M, YN), strip, NN)
    for s in range(n_facet):
        top = prod[2 * M * s : 2 * M * s + M]
        low = prod[2 * M * s + M : 2 * M * (s + 1)]
        contrib_out[s] = (top + minus_plus * swapped(low)).astype(BF16)
    for s in facet_order[:-1]:
        facet_copy(0, contrib_out, contrib_in, s, my_f, s).start()
    contrib_in[my_f] = contrib_out[my_f]

    pred_re = jnp.zeros((M, n_vis), F32)
    pred_im = jnp.zeros((M, n_vis), F32)
    for i in range(n_facet):
        f = facet_order[n_facet - 1 - i]
        if i > 0:
            facet_copy(0, contrib_out, contrib_in, f, f, f).wait_recv()
        with_re = dot(contrib_in[f], u_tab[f, :M], TN)
        with_im = dot(contrib_in[f], u_tab[f, M:], TN)
        rows_re = with_re[:M] - with_im[M:]
        rows_im = with_im[:M] + with_re[M:]
        v_re, v_im = v_tab[f, :M], v_tab[f, M:]
        pred_re += rows_re * v_re - rows_im * v_im
        pred_im += rows_re * v_im + rows_im * v_re
    pred_re = jnp.sum(pred_re, axis=0, keepdims=True)
    pred_im = jnp.sum(pred_im, axis=0, keepdims=True)
    predicted[0, 0, pl.ds(0, 1)] = pred_re
    predicted[0, 0, pl.ds(1, 1)] = pred_im
    weight = SUB / math.sqrt(n_vis)
    diff_re = pred_re - observed[0, 0, pl.ds(0, 1)]
    diff_im = pred_im - observed[0, 0, pl.ds(1, 1)]
    for i, f in enumerate(facet_order):
        v_re, v_im = v_tab[f, :M], v_tab[f, M:]
        wgt_re = ((diff_re * v_re + diff_im * v_im) * weight).astype(BF16)
        wgt_im = ((diff_im * v_re - diff_re * v_im) * weight).astype(BF16)
        prod = dot(u_tab[f], jnp.concatenate([wgt_re, wgt_im], axis=0), NT)
        part = (prod[:M] - minus_plus * swapped(prod[M:])).astype(BF16)
        if i < n_facet - 1:
            back_out[f] = part
            facet_copy(1, back_out, back_in, f, my_f, f).start()
        else:
            back_in[f] = part

    for s in facet_order[:-1]:
        facet_copy(1, back_out, back_in, s, s, s).wait_recv()
    stacked = []
    for s in range(n_facet):
        block = back_in[s]
        stacked += [block, (-minus_plus * swapped(block.astype(F32))).astype(BF16)]
    back_scale = math.sqrt(YN / (M * n_facet))
    stacked = jnp.concatenate(stacked, axis=0)
    for i, pair in enumerate(pair_order):
        start = pl.multiple_of(pair * (2 * n_rows), 2 * n_rows)
        delta = dot(subt_t[pl.ds(start, 2 * n_rows)], stacked, NN) * back_scale
        delta_out[pl.ds(2 * pair, 2)] = delta.reshape(2, n_rows, 2 * M).astype(BF16)
        for c in col_order[2 * i : 2 * i + 2]:
            if c is not col_order[-1]:
                col_copy(1, delta_out, delta_in, c, my_c, c).start()
    delta_in[my_c] = delta_out[my_c]

    up_scale = math.sqrt(YN / (M * n_col))
    for i in reversed(range(n_pair)):
        for c in col_order[2 * i : 2 * i + 2]:
            if c is not col_order[-1]:
                col_copy(1, delta_out, delta_in, c, c, c).wait_recv()
        pair = pair_order[i]
        blocks = [delta_in[2 * pair + core] for core in range(2)]
        turned = [(-minus_plus * swapped(block.astype(F32))).astype(BF16) for block in blocks]
        walls = wall[pl.ds(2 * pair, 2)].reshape(4 * M, YN)
        for part, sides in enumerate((blocks, turned)):
            term = dot(jnp.concatenate(sides, axis=1), walls, NN)
            if i < n_pair - 1:
                term += update[0, part]
            update[0, part] = term * up_scale if i == 0 else term

    for c in col_order[:-1]:
        col_copy(0, strip_out, strip_in, c, c, c).wait_send()
        col_copy(1, delta_out, delta_in, c, c, c).wait_send()
    for f in facet_order[:-1]:
        facet_copy(0, contrib_out, contrib_in, f, f, f).wait_send()
        facet_copy(1, back_out, back_in, f, f, f).wait_send()


def deliver_kernel(predicted, update, predicted_hbm, update_hbm, sems):
    copies = [
        pltpu.make_async_copy(update, update_hbm, sems.at[0]),
        pltpu.make_async_copy(predicted, predicted_hbm, sems.at[1]),
    ]
    for copy in copies:
        copy.start()
    for copy in copies:
        copy.wait()


def deliver(predicted, update):
    vmem = pl.BlockSpec(memory_space=pltpu.VMEM)
    hbm = pl.BlockSpec(memory_space=pltpu.HBM)
    return pl.pallas_call(
        deliver_kernel,
        out_shape=(
            jax.ShapeDtypeStruct(predicted.shape, F32),
            jax.ShapeDtypeStruct(update.shape, F32),
        ),
        in_specs=[vmem, vmem],
        out_specs=(hbm, hbm),
        scratch_shapes=[pltpu.SemaphoreType.DMA((2,))],
        compiler_params=pltpu.CompilerParams(vmem_limit_bytes=2**20),
        name="deliver",
    )(predicted, update)


def body(n_facet, n_col, facets, col_offsets, sub_rows, facet_offsets, vis_pos, observed):
    assert sub_rows.shape[0] == n_facet
    n_rows = facets.shape[2]
    n_vis = vis_pos.shape[3]
    vmem = pl.BlockSpec(memory_space=pltpu.VMEM)
    facet_blocks = pltpu.VMEM((n_facet, M, 2 * M), BF16)
    col_blocks = pltpu.VMEM((n_col, n_rows, 2 * M), BF16)
    table_rows = n_col + n_facet
    vmem_left = (67043328 - 4 * (facets.size + observed.size)) // 1024 * 1024 - MARGIN
    results = pl.pallas_call(
            functools.partial(kernel, n_facet, n_col),
            out_shape=(pltpu.VMEM(observed.shape, F32), pltpu.VMEM(facets.shape, F32)),
            in_specs=[pl.BlockSpec(memory_space=pltpu.HBM)] * 6,
            out_specs=(vmem, vmem),
            scratch_shapes=[
                pltpu.VMEM((2, n_rows, YN), BF16),
                pltpu.SMEM(col_offsets.shape, jnp.int32),
                pltpu.SMEM(sub_rows.shape[::-1], jnp.int32),
                pltpu.SMEM(facet_offsets.shape[::-1], jnp.int32),
                pltpu.VMEM(vis_pos.shape, jnp.int32),
                pltpu.VMEM(observed.shape, F32),
                pltpu.VMEM((2, M, YN), F32),
                pltpu.VMEM((2, table_rows, YN), F32),
                pltpu.VMEM((n_col, 2 * M, YN), BF16),
                pltpu.VMEM((n_facet, 2 * M, YN), BF16),
                pltpu.VMEM((YN, n_facet * 2 * M), BF16),
                pltpu.VMEM((n_facet, 2 * M, n_vis), BF16),
                pltpu.VMEM((n_facet, 2 * M, n_vis), F32),
                col_blocks,
                col_blocks,
                facet_blocks,
                facet_blocks,
                facet_blocks,
                facet_blocks,
                col_blocks,
                col_blocks,
                pltpu.SemaphoreType.DMA((6,)),
                pltpu.SemaphoreType.DMA((2, n_col)),
                pltpu.SemaphoreType.DMA((2, n_col)),
                pltpu.SemaphoreType.DMA((2, n_facet)),
                pltpu.SemaphoreType.DMA((2, n_facet)),
            ],
            compiler_params=pltpu.CompilerParams(
                collective_id=0, has_side_effects=True, vmem_limit_bytes=vmem_left
            ),
            name="predict_update",
        )(facets, col_offsets, sub_rows.T, facet_offsets.T, vis_pos, observed)
    return deliver(*results)


def solution(mesh):
    in_specs = (
        P("facet", None, "col", None),
        P(),
        P(None, "col"),
        P(),
        P("facet", "col", None, None),
        P("facet", "col", None, None),
    )
    out_specs = (P("facet", "col", None, None), P("facet", None, "col", None))
    step = functools.partial(body, mesh.shape["facet"], mesh.shape["col"])
    return jax.shard_map(step, mesh=mesh, in_specs=in_specs, out_specs=out_specs, check_vma=False)
```

```python
import functools
import math

import jax
import jax.numpy as jnp
from jax import lax
from jax.experimental import pallas as pl
from jax.experimental.pallas import tpu as pltpu
from jax.sharding import PartitionSpec as P

M = 64
SUB = 384
FINE = 1536
YN = 768
MARGIN = 8192
MESH = pl.DeviceIdType.MESH
F32 = jnp.float32
BF16 = jnp.bfloat16


def cis(product, modulus, direction):
    turns = jnp.floor(product * (1.0 / modulus) + 0.5)
    half = (product - turns * modulus) * (direction * math.pi / modulus)
    z = half * half
    s = half * (1.0 + z * (-1 / 6 + z * (1 / 120 + z * (-1 / 5040 + z * (1 / 362880 + z * (-1 / 39916800))))))
    c = 1.0 + z * (-1 / 2 + z * (1 / 24 + z * (-1 / 720 + z * (1 / 40320 + z * (-1 / 3628800 + z * (1 / 479001600))))))
    return 1.0 - 2.0 * s * s, 2.0 * s * c


def iota(shape, axis):
    return lax.broadcasted_iota(jnp.int32, shape, axis).astype(F32)


def dot(left, right, dims):
    return lax.dot_general(left, right, (dims, ((), ())), preferred_element_type=F32)


NN = ((1,), (0,))
NT = ((1,), (1,))
TN = ((0,), (0,))


def kernel(
    n_facet,
    n_col,
    facets_hbm,
    col_offsets_hbm,
    sub_rows_hbm,
    facet_offsets_hbm,
    vis_pos_hbm,
    observed_hbm,
    predicted,
    update,
    facet_buf,
    col_offsets,
    sub_rows,
    facet_offsets,
    vis_pos,
    observed,
    base,
    turn,
    wall,
    subt,
    subt_t,
    u_tab,
    v_tab,
    strip_out,
    strip_in,
    contrib_out,
    contrib_in,
    back_out,
    back_in,
    delta_out,
    delta_in,
    load_sem,
    col_send,
    col_recv,
    facet_send,
    facet_recv,
):
    my_f = lax.axis_index("facet")
    my_c = lax.axis_index("col")
    n_rows = facet_buf.shape[1]
    n_vis = vis_pos.shape[3]

    loads = [
        pltpu.make_async_copy(source, held, load_sem.at[i])
        for i, (source, held) in enumerate(
            (
                (col_offsets_hbm, col_offsets),
                (sub_rows_hbm, sub_rows),
                (facets_hbm.at[0], facet_buf),
                (facet_offsets_hbm, facet_offsets),
                (vis_pos_hbm, vis_pos),
                (observed_hbm, observed),
            )
        )
    ]
    for load in loads:
        load.start()
    barrier = pltpu.get_barrier_semaphore()
    n_pair = n_col // 2
    my_pair, my_core = my_c // 2, lax.rem(my_c, 2)
    side = my_pair // (n_pair // 2)
    mirrored = my_pair + side * (n_pair - 1 - 2 * my_pair)
    pair_order = []
    for place in range(n_pair - 1, 0, -1):
        target = place - (mirrored + n_pair - place) // n_pair
        pair_order.append(target + side * (n_pair - 1 - 2 * target))
    pair_order.append(my_pair)
    col_order = []
    for pair in pair_order:
        col_order += [2 * pair + 1 - my_core, 2 * pair + my_core]
    facet_order = [lax.rem(my_f + 1 + i, n_facet) for i in range(n_facet)]
    for c in col_order[:-1]:
        pl.semaphore_signal(barrier, inc=1, device_id=(my_f, c), device_id_type=MESH)
    for f in facet_order[:-1]:
        pl.semaphore_signal(barrier, inc=1, device_id=(f, my_c), device_id_type=MESH)

    def col_copy(phase, out, into, slot_out, slot_in, target):
        return pltpu.make_async_remote_copy(
            src_ref=out.at[slot_out],
            dst_ref=into.at[slot_in],
            send_sem=col_send.at[phase, slot_out],
            recv_sem=col_recv.at[phase, slot_in],
            device_id=(my_f, target),
            device_id_type=MESH,
        )

    def facet_copy(phase, out, into, slot_out, slot_in, target):
        return pltpu.make_async_remote_copy(
            src_ref=out.at[slot_out],
            dst_ref=into.at[slot_in],
            send_sem=facet_send.at[phase, slot_out],
            recv_sem=facet_recv.at[phase, slot_in],
            device_id=(target, my_c),
            device_id_type=MESH,
        )

    base_re, base_im = cis(iota((M, YN), 0) * iota((M, YN), 1), YN, -1.0)
    inv_root = 1.0 / math.sqrt(YN)
    base[0] = base_re * inv_root
    base[1] = base_im * inv_root
    along = iota((1, YN), 1)
    loads[0].wait()
    loads[1].wait()
    for c in range(n_col):
        turn[0, pl.ds(c, 1)] = along * col_offsets[c].astype(F32)
    for s in range(n_facet):
        turn[0, pl.ds(n_col + s, 1)] = along * sub_rows[0, s].astype(F32)
    turn_re, turn_im = cis(turn[0], YN, -1.0)
    turn[0] = turn_re
    turn[1] = turn_im

    def table(into, row, slot):
        re, im = turn[0, pl.ds(row, 1)], turn[1, pl.ds(row, 1)]
        into[slot, :M] = (base[0] * re - base[1] * im).astype(BF16)
        into[slot, M:] = (base[0] * im + base[1] * re).astype(BF16)

    lane = lax.broadcasted_iota(jnp.int32, (1, 2 * M), 1)
    minus_plus = jnp.where(lane < M, -1.0, 1.0)

    def swapped(value):
        return pltpu.roll(value, M, 1)

    loads[2].wait()
    both = facet_buf[...]
    if n_rows % 16:
        both = both.astype(F32).reshape(2 * n_rows, YN).astype(BF16)
    else:
        both = both.reshape(2 * n_rows, YN)
    early = n_col - 1
    for i, c in enumerate(col_order):
        table(wall, c, c)
        prod = dot(both, wall[c], NT)
        part = (prod[:n_rows] + minus_plus * swapped(prod[n_rows:])).astype(BF16)
        if i < n_col - 1:
            strip_out[c] = part
        else:
            strip_in[c] = part
        if i == early - 1:
            pl.semaphore_wait(barrier, n_col - 1 + n_facet - 1)
            for ready in col_order[:early]:
                col_copy(0, strip_out, strip_in, ready, my_c, ready).start()
        elif early <= i < n_col - 1:
            col_copy(0, strip_out, strip_in, c, my_c, c).start()

    for s in range(n_facet):
        table(subt, n_col + s, s)
    for load in loads[3:]:
        load.wait()
    for tab, which in ((u_tab, 0), (v_tab, 1)):
        point = vis_pos[0, 0, pl.ds(which, 1)].astype(F32)
        low_re, low_im = cis(iota((M, n_vis), 0) * point, FINE, 1.0)
        low_re = low_re * (1.0 / math.sqrt(SUB))
        low_im = low_im * (1.0 / math.sqrt(SUB))
        for f in range(n_facet):
            high_re, high_im = cis(point * facet_offsets[which, f].astype(F32), FINE, 1.0)
            tab[f, :M] = (low_re * high_re - low_im * high_im).astype(tab.dtype)
            tab[f, M:] = (low_re * high_im + low_im * high_re).astype(tab.dtype)
    for s in range(n_facet):
        subt_t[:, 2 * M * s : 2 * M * (s + 1)] = subt[s].T

    for c in col_order[:-1]:
        col_copy(0, strip_out, strip_in, c, c, c).wait_recv()
    strip = strip_in[...]
    if n_rows % 16:
        strip = strip.astype(F32).reshape(YN, 2 * M).astype(BF16)
    else:
        strip = strip.reshape(YN, 2 * M)
    for i, s in enumerate(facet_order):
        prod = dot(subt[s], strip, NN)
        part = (prod[:M] + minus_plus * swapped(prod[M:])).astype(BF16)
        if i < n_facet - 1:
            contrib_out[s] = part
            facet_copy(0, contrib_out, contrib_in, s, my_f, s).start()
        else:
            contrib_in[s] = part

    pred_re = jnp.zeros((M, n_vis), F32)
    pred_im = jnp.zeros((M, n_vis), F32)
    for i in range(n_facet):
        f = facet_order[n_facet - 1 - i]
        if i > 0:
            facet_copy(0, contrib_out, contrib_in, f, f, f).wait_recv()
        with_re = dot(contrib_in[f], u_tab[f, :M], TN)
        with_im = dot(contrib_in[f], u_tab[f, M:], TN)
        rows_re = with_re[:M] - with_im[M:]
        rows_im = with_im[:M] + with_re[M:]
        v_re, v_im = v_tab[f, :M], v_tab[f, M:]
        pred_re += rows_re * v_re - rows_im * v_im
        pred_im += rows_re * v_im + rows_im * v_re
    pred_re = jnp.sum(pred_re, axis=0, keepdims=True)
    pred_im = jnp.sum(pred_im, axis=0, keepdims=True)
    predicted[0, 0, pl.ds(0, 1)] = pred_re
    predicted[0, 0, pl.ds(1, 1)] = pred_im
    weight = SUB / math.sqrt(n_vis)
    diff_re = pred_re - observed[0, 0, pl.ds(0, 1)]
    diff_im = pred_im - observed[0, 0, pl.ds(1, 1)]
    for i, f in enumerate(facet_order):
        v_re, v_im = v_tab[f, :M], v_tab[f, M:]
        wgt_re = ((diff_re * v_re + diff_im * v_im) * weight).astype(BF16)
        wgt_im = ((diff_im * v_re - diff_re * v_im) * weight).astype(BF16)
        prod = dot(u_tab[f], jnp.concatenate([wgt_re, wgt_im], axis=0), NT)
        part = (prod[:M] - minus_plus * swapped(prod[M:])).astype(BF16)
        if i < n_facet - 1:
            back_out[f] = part
            facet_copy(1, back_out, back_in, f, my_f, f).start()
        else:
            back_in[f] = part

    for s in facet_order[:-1]:
        facet_copy(1, back_out, back_in, s, s, s).wait_recv()
    stacked = []
    for s in range(n_facet):
        block = back_in[s]
        stacked += [block, (-minus_plus * swapped(block.astype(F32))).astype(BF16)]
    back_scale = math.sqrt(YN / (M * n_facet))
    stacked = jnp.concatenate(stacked, axis=0)
    for i, pair in enumerate(pair_order):
        start = pl.multiple_of(pair * (2 * n_rows), 2 * n_rows)
        delta = dot(subt_t[pl.ds(start, 2 * n_rows)], stacked, NN) * back_scale
        delta_out[pl.ds(2 * pair, 2)] = delta.reshape(2, n_rows, 2 * M).astype(BF16)
        for c in col_order[2 * i : 2 * i + 2]:
            if c is not col_order[-1]:
                col_copy(1, delta_out, delta_in, c, my_c, c).start()
    delta_in[my_c] = delta_out[my_c]

    up_scale = math.sqrt(YN / (M * n_col))
    for i in reversed(range(n_pair)):
        for c in col_order[2 * i : 2 * i + 2]:
            if c is not col_order[-1]:
                col_copy(1, delta_out, delta_in, c, c, c).wait_recv()
        pair = pair_order[i]
        blocks = [delta_in[2 * pair + core] for core in range(2)]
        turned = [(-minus_plus * swapped(block.astype(F32))).astype(BF16) for block in blocks]
        walls = wall[pl.ds(2 * pair, 2)].reshape(4 * M, YN)
        for part, sides in enumerate((blocks, turned)):
            term = dot(jnp.concatenate(sides, axis=1), walls, NN)
            if i < n_pair - 1:
                term += update[0, part]
            update[0, part] = term * up_scale if i == 0 else term

    for c in col_order[:-1]:
        col_copy(0, strip_out, strip_in, c, c, c).wait_send()
        col_copy(1, delta_out, delta_in, c, c, c).wait_send()
    for f in facet_order[:-1]:
        facet_copy(0, contrib_out, contrib_in, f, f, f).wait_send()
        facet_copy(1, back_out, back_in, f, f, f).wait_send()


def deliver_kernel(predicted, update, predicted_hbm, update_hbm, sems):
    copies = [
        pltpu.make_async_copy(update, update_hbm, sems.at[0]),
        pltpu.make_async_copy(predicted, predicted_hbm, sems.at[1]),
    ]
    for copy in copies:
        copy.start()
    for copy in copies:
        copy.wait()


def deliver(predicted, update):
    vmem = pl.BlockSpec(memory_space=pltpu.VMEM)
    hbm = pl.BlockSpec(memory_space=pltpu.HBM)
    return pl.pallas_call(
        deliver_kernel,
        out_shape=(
            jax.ShapeDtypeStruct(predicted.shape, F32),
            jax.ShapeDtypeStruct(update.shape, F32),
        ),
        in_specs=[vmem, vmem],
        out_specs=(hbm, hbm),
        scratch_shapes=[pltpu.SemaphoreType.DMA((2,))],
        compiler_params=pltpu.CompilerParams(vmem_limit_bytes=2**20),
        name="deliver",
    )(predicted, update)


def body(n_facet, n_col, facets, col_offsets, sub_rows, facet_offsets, vis_pos, observed):
    assert sub_rows.shape[0] == n_facet
    n_rows = facets.shape[2]
    n_vis = vis_pos.shape[3]
    vmem = pl.BlockSpec(memory_space=pltpu.VMEM)
    facet_blocks = pltpu.VMEM((n_facet, M, 2 * M), BF16)
    col_blocks = pltpu.VMEM((n_col, n_rows, 2 * M), BF16)
    table_rows = n_col + n_facet
    vmem_left = (67043328 - 4 * (facets.size + observed.size)) // 1024 * 1024 - MARGIN
    results = pl.pallas_call(
            functools.partial(kernel, n_facet, n_col),
            out_shape=(pltpu.VMEM(observed.shape, F32), pltpu.VMEM(facets.shape, F32)),
            in_specs=[pl.BlockSpec(memory_space=pltpu.HBM)] * 6,
            out_specs=(vmem, vmem),
            scratch_shapes=[
                pltpu.VMEM((2, n_rows, YN), BF16),
                pltpu.SMEM(col_offsets.shape, jnp.int32),
                pltpu.SMEM(sub_rows.shape[::-1], jnp.int32),
                pltpu.SMEM(facet_offsets.shape[::-1], jnp.int32),
                pltpu.VMEM(vis_pos.shape, jnp.int32),
                pltpu.VMEM(observed.shape, F32),
                pltpu.VMEM((2, M, YN), F32),
                pltpu.VMEM((2, table_rows, YN), F32),
                pltpu.VMEM((n_col, 2 * M, YN), BF16),
                pltpu.VMEM((n_facet, 2 * M, YN), BF16),
                pltpu.VMEM((YN, n_facet * 2 * M), BF16),
                pltpu.VMEM((n_facet, 2 * M, n_vis), BF16),
                pltpu.VMEM((n_facet, 2 * M, n_vis), F32),
                col_blocks,
                col_blocks,
                facet_blocks,
                facet_blocks,
                facet_blocks,
                facet_blocks,
                col_blocks,
                col_blocks,
                pltpu.SemaphoreType.DMA((6,)),
                pltpu.SemaphoreType.DMA((2, n_col)),
                pltpu.SemaphoreType.DMA((2, n_col)),
                pltpu.SemaphoreType.DMA((2, n_facet)),
                pltpu.SemaphoreType.DMA((2, n_facet)),
            ],
            compiler_params=pltpu.CompilerParams(
                collective_id=0, has_side_effects=True, vmem_limit_bytes=vmem_left
            ),
            name="predict_update",
        )(facets, col_offsets, sub_rows.T, facet_offsets.T, vis_pos, observed)
    return deliver(*results)


def solution(mesh):
    in_specs = (
        P("facet", None, "col", None),
        P(),
        P(None, "col"),
        P(),
        P("facet", "col", None, None),
        P("facet", "col", None, None),
    )
    out_specs = (P("facet", "col", None, None), P("facet", None, "col", None))
    step = functools.partial(body, mesh.shape["facet"], mesh.shape["col"])
    return jax.shard_map(step, mesh=mesh, in_specs=in_specs, out_specs=out_specs, check_vma=False)
```
